128 devices in a mesh: pr: 16 (over z_lo, y, core), pc: 8 (over z_hi, x).
Axes of the slice: x: 4, y: 4, z: 4 (z_hi: 2, z_lo: 2; z = z_hi * 2 + z_lo), core: 2. Of those that a mesh axis runs over, the one named last changes fastest.
Arguments:
- pair_array: bfloat16 [1024, 1024, 128], P('pr', 'pc'), may hold values from -6 to 6
- left_weight: bfloat16 [128, 128], replicated, may hold values from -0.5 to 0.5
- right_weight: bfloat16 [128, 128], replicated, may hold values from -0.5 to 0.5
- left_gate: bfloat16 [128, 128], replicated, may hold values from -0.5 to 0.5
- right_gate: bfloat16 [128, 128], replicated, may hold values from -0.5 to 0.5
- mid_gain: float32 [128], replicated, may hold values from 0.25 to 1.75
- out_weight: bfloat16 [128, 128], replicated, may hold values from -0.5 to 0.5
- out_gate: bfloat16 [128, 128], replicated, may hold values from -0.5 to 0.5
Outputs:
- pair_update: bfloat16 [1024, 1024, 128], P('pr', 'pc')
The draws below stay inside these ranges and needn't reach their ends.
All inputs are finite; a program needn't handle non-finite values.
Results may differ from the reference program's by a relative error of at most 0.012.
Values may be sent and summed in bfloat16 or wider, within the bound.
A program may use at most 128 MiB of HBM per device.

```python
import jax
import jax.numpy as jnp
from jax import lax

RESIDUES = 1024
PAIR_WIDTH = 128
MIX_WIDTH = 128


def shard_levels(rng, extent, pieces, least, largest):
    loudness = 1.0
    for axis_at, parts in pieces:
        draws = jax.random.uniform(jax.random.fold_in(jax.random.fold_in(rng, 6), axis_at), (parts,), jnp.float32, least / len(pieces), largest / len(pieces))
        loudness = loudness * jnp.repeat(jnp.exp(draws), extent[axis_at] // parts).reshape((-1,) + (1,) * (len(extent) - 1 - axis_at))
    return loudness


def bell_draw(key, shape, scale, reach, pieces=(), dtype=jnp.bfloat16):
    entries = jax.random.normal(key, shape, jnp.float32) * scale
    if len(pieces) > 0:
        entries = shard_levels(key, shape, pieces, -0.22, 0.18) * entries
    return jnp.clip(entries, min=-reach, max=reach).astype(dtype)


def setup_inputs(seed: int = 0) -> dict:
    keys = jax.random.split(jax.random.key(seed), 9)
    pair_array = bell_draw(keys[0], (RESIDUES, RESIDUES, PAIR_WIDTH), 1.0, 6.0, ((0, 16), (1, 8)))
    left_weight = bell_draw(keys[1], (PAIR_WIDTH, MIX_WIDTH), PAIR_WIDTH ** -0.5, 0.5)
    right_weight = bell_draw(keys[2], (PAIR_WIDTH, MIX_WIDTH), PAIR_WIDTH ** -0.5, 0.5)
    left_gate = bell_draw(keys[3], (PAIR_WIDTH, MIX_WIDTH), PAIR_WIDTH ** -0.5, 0.5)
    right_gate = bell_draw(keys[4], (PAIR_WIDTH, MIX_WIDTH), PAIR_WIDTH ** -0.5, 0.5)
    mid_gain = jnp.clip(1.0 + 0.15 * jax.random.normal(keys[5], (MIX_WIDTH,), jnp.float32), 0.25, 1.75)
    out_weight = bell_draw(keys[6], (MIX_WIDTH, PAIR_WIDTH), MIX_WIDTH ** -0.5, 0.5)
    out_gate = bell_draw(keys[7], (PAIR_WIDTH, PAIR_WIDTH), PAIR_WIDTH ** -0.5, 0.5)
    return {"pair_array": pair_array, "left_weight": left_weight, "right_weight": right_weight, "left_gate": left_gate, "right_gate": right_gate, "mid_gain": mid_gain, "out_weight": out_weight, "out_gate": out_gate}


def unit_channels(values, channel_gain):
    centred = values - lax.optimization_barrier(jnp.mean(values, axis=-1, keepdims=True))
    return centred * lax.rsqrt(lax.optimization_barrier(jnp.mean(centred * centred, axis=-1, keepdims=True)) + 1e-05) * channel_gain

def make_factors(pair_in, left_weight, right_weight, left_gate, right_gate):
    ready = pair_in
    left = jnp.einsum('ijc,cd->ijd', ready.astype(jnp.float32), left_weight.astype(jnp.float32))
    left = left * jax.nn.sigmoid(jnp.einsum('ijc,cd->ijd', ready.astype(jnp.float32), left_gate.astype(jnp.float32)))
    right = jnp.einsum('ijc,cd->ijd', ready.astype(jnp.float32), right_weight.astype(jnp.float32))
    right = right * jax.nn.sigmoid(jnp.einsum('ijc,cd->ijd', ready.astype(jnp.float32), right_gate.astype(jnp.float32)))
    return (ready, left.astype(jnp.bfloat16), right.astype(jnp.bfloat16))

def to_pair(mixed, ready, mid_gain, out_weight, out_gate):
    scaled = unit_channels(mixed.astype(jnp.float32), mid_gain).astype(jnp.bfloat16)
    scaled = lax.optimization_barrier(scaled)
    gate = jax.nn.sigmoid(jnp.einsum('ijc,cd->ijd', ready.astype(jnp.float32), out_gate.astype(jnp.float32)))
    return (jnp.einsum('ijd,dc->ijc', scaled.astype(jnp.float32), out_weight.astype(jnp.float32)) * gate).astype(jnp.bfloat16)

def reference(pair_array, left_weight, right_weight, left_gate, right_gate, mid_gain, out_weight, out_gate):
    ready, left, right = make_factors(pair_array, left_weight, right_weight, left_gate, right_gate)
    left, right = lax.optimization_barrier((left, right))

    def one_channel(pair_of):
        return (jnp.dot(pair_of[0].T, pair_of[1], preferred_element_type=jnp.float32) * RESIDUES ** (-0.5)).astype(jnp.bfloat16)
    mixed = jnp.moveaxis(lax.map(one_channel, (jnp.moveaxis(left, -1, 0), jnp.moveaxis(right, -1, 0))), 0, -1)
    mixed = lax.optimization_barrier(mixed)
    return to_pair(mixed, ready, mid_gain, out_weight, out_gate)
```

```python
import jax
import jax.numpy as jnp
from jax import lax
from jax.sharding import PartitionSpec as P

BOTH = ("pr", "pc")


def factor(pair_in, weight, gate):
    value = jnp.einsum("ijc,cd->ijd", pair_in, weight, preferred_element_type=jnp.float32)
    value = value * jax.nn.sigmoid(
        jnp.einsum("ijc,cd->ijd", pair_in, gate, preferred_element_type=jnp.float32)
    )
    return value.astype(jnp.bfloat16)


def on_device(
    pair_array, left_weight, right_weight, left_gate, right_gate, mid_gain, out_weight, out_gate
):
    rows, columns, _ = pair_array.shape
    pr, pc = lax.axis_size("pr"), lax.axis_size("pc")
    count = rows * pr
    left = factor(pair_array, left_weight, left_gate)
    right = factor(pair_array, right_weight, right_gate)
    left = lax.all_to_all(jnp.moveaxis(left, 2, 0), BOTH, split_axis=0, concat_axis=0, tiled=True)
    right = lax.all_to_all(jnp.moveaxis(right, 2, 0), BOTH, split_axis=0, concat_axis=0, tiled=True)
    left = left.reshape(pr, pc, rows, columns)
    right = right.reshape(pr, pc, rows, columns)
    left = jnp.moveaxis(left, 1, 2).reshape(count, count)
    right = jnp.moveaxis(right, 1, 2).reshape(count, count)
    mixed = jnp.einsum("ki,kj->ij", left, right, preferred_element_type=jnp.float32)
    mixed = (mixed * count ** (-0.5)).astype(jnp.bfloat16)
    mixed = jnp.moveaxis(mixed.reshape(pr, rows, pc, columns), 2, 1).reshape(pr * pc, rows, columns)
    mixed = lax.all_to_all(mixed, BOTH, split_axis=0, concat_axis=0, tiled=True)
    values = mixed.astype(jnp.float32)
    centred = values - jnp.mean(values, axis=0, keepdims=True)
    scaled = (
        centred
        * lax.rsqrt(jnp.mean(centred * centred, axis=0, keepdims=True) + 1e-05)
        * mid_gain[:, None, None]
    ).astype(jnp.bfloat16)
    gate = jax.nn.sigmoid(
        jnp.einsum("ijc,cd->ijd", pair_array, out_gate, preferred_element_type=jnp.float32)
    )
    return (
        jnp.einsum("dij,dc->ijc", scaled, out_weight, preferred_element_type=jnp.float32) * gate
    ).astype(jnp.bfloat16)


def solution(mesh):
    return jax.shard_map(
        on_device,
        mesh=mesh,
        in_specs=(P("pr", "pc", None), P(), P(), P(), P(), P(), P(), P()),
        out_specs=P("pr", "pc", None),
        check_vma=False,
    )
```

```python
import functools

import jax
import jax.numpy as jnp
from jax import lax
from jax.experimental import pallas as pl
from jax.experimental.pallas import tpu as pltpu
from jax.sharding import PartitionSpec as P

MESH = pl.DeviceIdType.MESH


def position():
    pr, pc = lax.axis_index("pr"), lax.axis_index("pc")
    return pc % 4, (pr // 2) % 4, (pc // 4) * 2 + pr // 8, pr % 2


def device(x, y, z, c):
    return ((z % 2) * 4 + y) * 2 + c, (z // 2) * 4 + x


def partner(here, code, parity):
    x, y, z, c = here
    dx, dy, dz, dc = 2 * (code % 2) + parity, (code // 2) % 4, (code // 8) % 4, code // 32
    return device((x + dx) % 4, (y + dy) % 4, (z + dz) % 4, (c + dc) % 2)


def exchange_kernel(
    scale, left_ref, right_ref, out_ref, lines, strips, sums, send_sem, recv_sem
):
    here = position()
    x = here[0]
    pr, pc = lax.axis_index("pr"), lax.axis_index("pc")
    mine = pr * 8 + pc
    slot = (pc // 4) * 2 + x // 2

    barrier = pltpu.get_barrier_semaphore()

    def greet(parity):
        def body(code, carry):
            pl.semaphore_signal(
                barrier, inc=1, device_id=partner(here, code, parity), device_id_type=MESH
            )
            return carry

        return body

    lax.fori_loop(1, 64, greet(0), 0)
    lax.fori_loop(0, 64, greet(1), 0)
    pl.semaphore_wait(barrier, 127)

    def send(source, target, index, to):
        pltpu.make_async_remote_copy(
            source, target, send_sem.at[index], recv_sem.at[index], device_id=to, device_id_type=MESH
        ).start()

    row, column = pl.multiple_of(pr * 64, 64), pl.multiple_of(pc * 128, 128)
    across = pl.multiple_of(slot * 128, 128)

    def send_left(parity):
        def body(step, carry):
            to = partner(here, (step * 37) % 64, parity)
            send(
                left_ref.at[to[0] * 8 + to[1]],
                lines.at[pl.ds(row, 64), pl.ds(column, 128)],
                0,
                to,
            )
            return carry

        return body

    def send_right(parity):
        def body(step, carry):
            to = partner(here, (step * 37) % 64, parity)
            send(
                right_ref.at[to[0] * 8 + to[1]],
                strips.at[parity, pl.ds(row, 64), pl.ds(across, 128)],
                1 + parity,
                to,
            )
            return carry

        return body

    def send_sums(parity):
        def body(step, carry):
            to = partner(here, (step * 37) % 64, parity)
            place = (to[1] // 4) * 2 + (to[1] % 4) // 2
            send(
                sums.at[parity, place, pl.ds(pl.multiple_of(to[0] * 64, 64), 64)],
                out_ref.at[mine],
                3 + parity,
                to,
            )
            return carry

        return body

    lax.fori_loop(1, 64, send_left(0), 0)
    lax.fori_loop(0, 64, send_left(1), 0)
    lax.fori_loop(1, 64, send_right(0), 0)
    lax.fori_loop(0, 64, send_right(1), 0)
    lines[pl.ds(row, 64), pl.ds(column, 128)] = left_ref[mine]
    strips[0, pl.ds(row, 64), pl.ds(across, 128)] = right_ref[mine]

    whole = (
        lines.at[pl.ds(0, 1016)],
        strips.at[0, pl.ds(0, 1008)],
        strips.at[1],
        sums.at[0, 0, pl.ds(0, 1008)],
        sums.at[0, 0],
    )
    parts = (1, 1, 1, 4, 4)

    def settle(sem, index):
        pltpu.make_async_copy(whole[index], whole[index], sem.at[index]).wait()

    settle(recv_sem, 0)
    for parity in (0, 1):
        settle(recv_sem, 1 + parity)

        def block(at, carry):
            start = pl.multiple_of(at * 128, 128)
            product = lax.dot_general(
                lines[:, pl.ds(start, 128)],
                strips[parity],
                (((0,), (0,)), ((), ())),
                preferred_element_type=jnp.float32,
            )
            product = (product * scale).astype(jnp.bfloat16)
            for place in range(4):
                sums[parity, place, pl.ds(start, 128)] = product[:, place * 128 : place * 128 + 128]
            return carry

        lax.fori_loop(0, 8, block, 0)
        if parity == 0:
            lax.fori_loop(1, 64, send_sums(0), 0)
        else:
            lax.fori_loop(0, 64, send_sums(1), 0)
    out_ref[mine] = sums[0, slot, pl.ds(row, 64)]

    for sem in (recv_sem, send_sem):
        pltpu.make_async_copy(out_ref.at[pl.ds(0, 63)], out_ref.at[pl.ds(0, 63)], sem.at[3]).wait()
        pltpu.make_async_copy(out_ref.at[pl.ds(0, 64)], out_ref.at[pl.ds(0, 64)], sem.at[4]).wait()
    for index in range(3):
        settle(send_sem, index)


def exchange(left, right):
    return pl.pallas_call(
        functools.partial(exchange_kernel, 1024 ** (-0.5)),
        out_shape=jax.ShapeDtypeStruct(left.shape, left.dtype),
        in_specs=[pl.BlockSpec(memory_space=pltpu.VMEM)] * 2,
        out_specs=pl.BlockSpec(memory_space=pltpu.VMEM),
        scratch_shapes=[
            pltpu.VMEM((1024, 1024), jnp.bfloat16),
            pltpu.VMEM((2, 1024, 512), jnp.bfloat16),
            pltpu.VMEM((2, 4, 1024, 128), jnp.bfloat16),
            pltpu.SemaphoreType.DMA((5,)),
            pltpu.SemaphoreType.DMA((5,)),
        ],
        compiler_params=pltpu.CompilerParams(
            collective_id=0, has_side_effects=True, vmem_limit_bytes=32 * 1024 * 1024
        ),
        name="exchange",
    )(left, right)


def factor(pair_in, weight, gate):
    value = jnp.einsum("ijc,cd->ijd", pair_in, weight, preferred_element_type=jnp.float32)
    value = value * jax.nn.sigmoid(
        jnp.einsum("ijc,cd->ijd", pair_in, gate, preferred_element_type=jnp.float32)
    )
    return jnp.moveaxis(value.astype(jnp.bfloat16), 2, 0)


def on_device(
    pair_array, left_weight, right_weight, left_gate, right_gate, mid_gain, out_weight, out_gate
):
    mixed = exchange(
        factor(pair_array, left_weight, left_gate), factor(pair_array, right_weight, right_gate)
    )
    values = mixed.astype(jnp.float32)
    centred = values - jnp.mean(values, axis=0, keepdims=True)
    scaled = (
        centred
        * lax.rsqrt(jnp.mean(centred * centred, axis=0, keepdims=True) + 1e-05)
        * mid_gain[:, None, None]
    ).astype(jnp.bfloat16)
    gate = jax.nn.sigmoid(
        jnp.einsum("ijc,cd->ijd", pair_array, out_gate, preferred_element_type=jnp.float32)
    )
    return (
        jnp.einsum("dij,dc->ijc", scaled, out_weight, preferred_element_type=jnp.float32) * gate
    ).astype(jnp.bfloat16)


def solution(mesh):
    return jax.shard_map(
        on_device,
        mesh=mesh,
        in_specs=(P("pr", "pc", None), P(), P(), P(), P(), P(), P(), P()),
        out_specs=P("pr", "pc", None),
        check_vma=False,
    )
```

```python
import functools

import jax
import jax.numpy as jnp
from jax import lax
from jax.experimental import pallas as pl
from jax.experimental.pallas import tpu as pltpu
from jax.sharding import PartitionSpec as P

MESH = pl.DeviceIdType.MESH


def position():
    pr, pc = lax.axis_index("pr"), lax.axis_index("pc")
    return pc % 4, (pr // 2) % 4, (pc // 4) * 2 + pr // 8, pr % 2


def device(x, y, z, c):
    return ((z % 2) * 4 + y) * 2 + c, (z // 2) * 4 + x


def partner(here, code, parity):
    x, y, z, c = here
    dx, dy, dz, dc = 2 * (code % 2) + parity, (code // 2) % 4, (code // 8) % 4, code // 32
    return device((x + dx) % 4, (y + dy) % 4, (z + dz) % 4, (c + dc) % 2)


def triangle_kernel(
    scale,
    pair_hbm,
    left_weight,
    right_weight,
    left_gate,
    right_gate,
    gain_ref,
    out_weight,
    out_gate,
    out_ref,
    pair,
    turned,
    gains,
    stage,
    left_send,
    right_send,
    lines,
    strips,
    sums,
    mixed,
    gate,
    load_sem,
    send_sem,
    recv_sem,
):
    here = position()
    x = here[0]
    pr, pc = lax.axis_index("pr"), lax.axis_index("pc")
    mine = pr * 8 + pc
    slot = (pc // 4) * 2 + x // 2
    row, column = pl.multiple_of(pr * 64, 64), pl.multiple_of(pc * 128, 128)
    across = pl.multiple_of(slot * 128, 128)

    load = pltpu.make_async_copy(pair_hbm, pair, load_sem)
    load.start()
    barrier = pltpu.get_barrier_semaphore()

    def partners(visit):
        def even(step, carry):
            visit(0, partner(here, (step * 37) % 64, 0))
            return carry

        def odd(step, carry):
            visit(1, partner(here, (step * 37) % 64, 1))
            return carry

        return lambda: lax.fori_loop(1, 64, even, 0), lambda: lax.fori_loop(0, 64, odd, 0)

    def greet(parity, to):
        pl.semaphore_signal(barrier, inc=1, device_id=to, device_id_type=MESH)

    for run in partners(greet):
        run()

    def send(source, target, index, to):
        pltpu.make_async_remote_copy(
            source, target, send_sem.at[index], recv_sem.at[index], device_id=to, device_id_type=MESH
        ).start()

    for index, ref in enumerate((left_weight, left_gate, right_weight, right_gate)):
        turned[index] = ref[...].astype(jnp.float32).T.astype(jnp.bfloat16)
    gains[...] = jnp.broadcast_to(gain_ref[...], (128, 128)).T

    def factor(index, first, target):
        for pair_at in range(8):
            both = pair[pl.ds(first + 2 * pair_at, 2)].reshape(256, 128)
            value = lax.dot_general(
                turned[index], both, (((1,), (1,)), ((), ())), preferred_element_type=jnp.float32
            )
            level = lax.dot_general(
                turned[index + 1], both, (((1,), (1,)), ((), ())), preferred_element_type=jnp.float32
            )
            value = value * jax.nn.sigmoid(level)
            stage[2 * pair_at] = value[:, :128]
            stage[2 * pair_at + 1] = value[:, 128:]

        def turn(at, carry):
            channel = pl.multiple_of(at * 8, 8)
            target[pl.ds(channel, 8)] = jnp.swapaxes(stage[:16, pl.ds(channel, 8), :], 0, 1).astype(
                jnp.bfloat16
            )
            return carry

        lax.fori_loop(0, 16, turn, 0)

    load.wait()
    for half in range(2):

        def left_rows(at, carry):
            start = pl.multiple_of(at * 16, 16)
            factor(0, half * 32 + start, left_send.at[half, :, pl.ds(start, 16)])
            return carry

        lax.fori_loop(0, 2, left_rows, 0)
        if half == 0:
            pl.semaphore_wait(barrier, 127)

        def send_left(parity, to):
            send(
                left_send.at[half, to[0] * 8 + to[1]],
                lines.at[pl.ds(pl.multiple_of(row + half * 32, 32), 32), pl.ds(column, 128)],
                half,
                to,
            )

        for run in partners(send_left):
            run()

    def right_rows(at, carry):
        start = pl.multiple_of(at * 16, 16)
        factor(2, start, right_send.at[:, pl.ds(start, 16)])
        return carry

    lax.fori_loop(0, 4, right_rows, 0)

    def send_right(parity, to):
        send(
            right_send.at[to[0] * 8 + to[1]],
            strips.at[parity, pl.ds(row, 64), pl.ds(across, 128)],
            2 + parity,
            to,
        )

    for run in partners(send_right):
        run()

    lines[pl.ds(row, 32), pl.ds(column, 128)] = left_send[0, mine]
    lines[pl.ds(pl.multiple_of(row + 32, 32), 32), pl.ds(column, 128)] = left_send[1, mine]
    strips[0, pl.ds(row, 64), pl.ds(across, 128)] = right_send[mine]

    def gate_rows(at, carry):
        start = at * 4
        level = jnp.dot(
            pair[pl.ds(start, 4)].reshape(512, 128),
            out_gate[...],
            preferred_element_type=jnp.float32,
        )
        gate[pl.ds(start, 4)] = jax.nn.sigmoid(level).reshape(4, 128, 128)
        return carry

    lax.fori_loop(0, 16, gate_rows, 0)

    def settle(ref, sem):
        pltpu.make_async_copy(ref, ref, sem).wait()

    settle(left_send.at[0, pl.ds(0, 127)], recv_sem.at[0])
    settle(left_send.at[1, pl.ds(0, 127)], recv_sem.at[1])
    for parity in (0, 1):
        settle(strips.at[parity, pl.ds(0, 1008 + 16 * parity)], recv_sem.at[2 + parity])

        def block(at, carry):
            start = pl.multiple_of(at * 128, 128)
            product = lax.dot_general(
                lines[:, pl.ds(start, 128)],
                strips[parity],
                (((0,), (0,)), ((), ())),
                preferred_element_type=jnp.float32,
            )
            product = (product * scale).astype(jnp.bfloat16)
            for place in range(4):
                sums[parity, place, pl.ds(start, 128)] = product[:, place * 128 : place * 128 + 128]
            return carry

        lax.fori_loop(0, 8, block, 0)

        for first, size, index in ((0, 64, 4),) if parity == 0 else ((0, 32, 5), (32, 32, 6)):

            def send_sums(_, to):
                place = (to[1] // 4) * 2 + (to[1] % 4) // 2
                send(
                    sums.at[parity, place, pl.ds(pl.multiple_of(to[0] * 64 + first, size), size)],
                    mixed.at[mine, pl.ds(first, size)],
                    index,
                    to,
                )

            partners(send_sums)[parity]()
    mixed[mine] = sums[0, slot, pl.ds(row, 64)]

    def finish(at, carry):
        start = pl.multiple_of(at * 16, 16)

        def turn(group, carry):
            channel = pl.multiple_of(group * 8, 8)
            stage[:, pl.ds(channel, 8), :] = jnp.swapaxes(
                mixed[pl.ds(channel, 8), pl.ds(start, 16), :].astype(jnp.float32), 0, 1
            )
            return carry

        lax.fori_loop(0, 16, turn, 0)

        def line(inner, carry):
            values = stage[inner]
            centred = values - jnp.mean(values, axis=0, keepdims=True)
            spread = lax.rsqrt(jnp.mean(centred * centred, axis=0, keepdims=True) + 1e-05)
            scaled = (centred * spread * gains[...]).astype(jnp.bfloat16)
            product = lax.dot_general(
                scaled,
                out_weight[...],
                (((0,), (0,)), ((), ())),
                preferred_element_type=jnp.float32,
            )
            out_ref[start + inner] = (product * gate[start + inner]).astype(jnp.bfloat16)
            return carry

        lax.fori_loop(0, 16, line, 0, unroll=4)
        return carry

    settle(mixed.at[pl.ds(0, 63)], recv_sem.at[4])
    settle(mixed.at[pl.ds(0, 32)], recv_sem.at[5])
    lax.fori_loop(0, 2, finish, 0)
    settle(mixed.at[pl.ds(0, 32)], recv_sem.at[6])
    lax.fori_loop(2, 4, finish, 0)

    settle(left_send.at[0, pl.ds(0, 127)], send_sem.at[0])
    settle(left_send.at[1, pl.ds(0, 127)], send_sem.at[1])
    settle(strips.at[0, pl.ds(0, 1008)], send_sem.at[2])
    settle(strips.at[1], send_sem.at[3])
    settle(mixed.at[pl.ds(0, 63)], send_sem.at[4])
    settle(mixed.at[pl.ds(0, 32)], send_sem.at[5])
    settle(mixed.at[pl.ds(0, 32)], send_sem.at[6])


def on_device(
    pair_array, left_weight, right_weight, left_gate, right_gate, mid_gain, out_weight, out_gate
):
    half, single = jnp.bfloat16, jnp.float32
    return pl.pallas_call(
        functools.partial(triangle_kernel, 1024 ** (-0.5)),
        out_shape=jax.ShapeDtypeStruct(pair_array.shape, half),
        in_specs=[pl.BlockSpec(memory_space=pl.ANY)] + [pl.BlockSpec(memory_space=pltpu.VMEM)] * 7,
        out_specs=pl.BlockSpec(memory_space=pltpu.VMEM),
        scratch_shapes=[
            pltpu.VMEM((64, 128, 128), half),
            pltpu.VMEM((4, 128, 128), half),
            pltpu.VMEM((128, 128), single),
            pltpu.VMEM((16, 128, 128), single),
            pltpu.VMEM((2, 128, 32, 128), half),
            pltpu.VMEM((128, 64, 128), half),
            pltpu.VMEM((1024, 1024), half),
            pltpu.VMEM((2, 1024, 512), half),
            pltpu.VMEM((2, 4, 1024, 128), half),
            pltpu.VMEM((128, 64, 128), half),
            pltpu.VMEM((64, 128, 128), single),
            pltpu.SemaphoreType.DMA,
            pltpu.SemaphoreType.DMA((7,)),
            pltpu.SemaphoreType.DMA((7,)),
        ],
        compiler_params=pltpu.CompilerParams(
            collective_id=0, has_side_effects=True, vmem_limit_bytes=48 * 1024 * 1024
        ),
        name="triangle",
    )(
        pair_array,
        left_weight,
        right_weight,
        left_gate,
        right_gate,
        mid_gain.reshape(1, 128),
        out_weight,
        out_gate,
    )


def solution(mesh):
    return jax.shard_map(
        on_device,
        mesh=mesh,
        in_specs=(P("pr", "pc", None), P(), P(), P(), P(), P(), P(), P()),
        out_specs=P("pr", "pc", None),
        check_vma=False,
    )
```

```python
import functools

import jax
import jax.numpy as jnp
from jax import lax
from jax.experimental import pallas as pl
from jax.experimental.pallas import tpu as pltpu
from jax.sharding import PartitionSpec as P

MESH = pl.DeviceIdType.MESH


def offsets():
    def negated(o):
        return tuple(-v % 4 for v in o)

    seen, sets = set(), []
    for code in range(64):
        o = (code // 16, code // 4 % 4, code % 4)
        if o in seen:
            continue
        one = []
        for _ in range(3):
            for p in (o, negated(o)):
                if p not in one:
                    one.append(p)
            o = (o[2], o[0], o[1])
        seen.update(one)
        sets.append(one)
    sets.sort(key=lambda one: -sum(min(v, 4 - v) for v in one[0]))
    flat = [o for one in sets for o in one]
    order = [(*o, (at + turn) % 2) for turn in (0, 1) for at, o in enumerate(flat)]
    return [o for o in order if o != (0, 0, 0, 0)]


ORDER = offsets()
SIDES = [[o for o in ORDER if o[0] % 2 == parity] for parity in (0, 1)]


def triangle_kernel(
    scale,
    pair_hbm,
    left_weight_hbm,
    right_weight_hbm,
    left_gate_hbm,
    right_gate_hbm,
    gain_hbm,
    out_weight_hbm,
    out_gate_hbm,
    out_ref,
    pair,
    weights,
    gain_row,
    turned,
    gains,
    stage,
    left_send,
    right_send,
    lines,
    strips,
    sums,
    mixed,
    gate,
    load_sem,
    send_sem,
    recv_sem,
):
    pr, pc = lax.axis_index("pr"), lax.axis_index("pc")
    x, y, c = lax.rem(pc, 4), lax.rem(lax.div(pr, 2), 4), lax.rem(pr, 2)
    z = lax.div(pc, 4) * 2 + lax.div(pr, 8)
    mine = pr * 8 + pc
    slot = lax.div(pc, 4) * 2 + lax.div(x, 2)
    xs = [lax.rem(x + d, 4) for d in range(4)]
    ys = [lax.rem(y + d, 4) * 2 for d in range(4)]
    zs = [lax.rem(z + d, 4) for d in range(4)]
    rows_of = [[lax.rem(v, 2) * 8 + w for w in ys] for v in zs]
    columns_of = [[lax.div(v, 2) * 4 + w for w in xs] for v in zs]
    places_of = [[lax.div(v, 2) * 2 + lax.div(w, 2) for w in xs] for v in zs]
    cores = [c, 1 - c]

    def partner(o):
        dx, dy, dz, dc = o
        return rows_of[dz][dy] + cores[dc], columns_of[dz][dx]

    row, column = pl.multiple_of(pr * 64, 64), pl.multiple_of(pc * 128, 128)
    across = pl.multiple_of(slot * 128, 128)

    matrices = (
        left_weight_hbm,
        left_gate_hbm,
        right_weight_hbm,
        right_gate_hbm,
        out_weight_hbm,
        out_gate_hbm,
    )
    loads = [
        pltpu.make_async_copy(ref, weights.at[index], load_sem.at[index])
        for index, ref in enumerate(matrices)
    ]
    loads.append(pltpu.make_async_copy(gain_hbm, gain_row, load_sem.at[6]))
    pair_loads = [
        pltpu.make_async_copy(
            pair_hbm.at[pl.ds(first, 32)], pair.at[pl.ds(first, 32)], load_sem.at[7 + first // 32]
        )
        for first in (0, 32)
    ]
    for load in loads + pair_loads:
        load.start()
    barrier = pltpu.get_barrier_semaphore()

    with jax.named_scope("greet"):
        for o in ORDER:
            pl.semaphore_signal(barrier, inc=1, device_id=partner(o), device_id_type=MESH)

    def send(source, target, index, to):
        pltpu.make_async_remote_copy(
            source, target, send_sem.at[index], recv_sem.at[index], device_id=to, device_id_type=MESH
        ).start()

    with jax.named_scope("weights"):
        for load in loads:
            load.wait()
        for index in range(4):
            turned[index] = weights[index].astype(jnp.float32).T.astype(jnp.bfloat16)
        gains[...] = jnp.broadcast_to(gain_row[...], (128, 128)).T

    def factor(index, first, target):
        for pair_at in range(8):
            both = pair[pl.ds(first + 2 * pair_at, 2)].reshape(256, 128)
            value = lax.dot_general(
                turned[index], both, (((1,), (1,)), ((), ())), preferred_element_type=jnp.float32
            )
            level = lax.dot_general(
                turned[index + 1], both, (((1,), (1,)), ((), ())), preferred_element_type=jnp.float32
            )
            value = value * jax.nn.sigmoid(level)
            stage[2 * pair_at] = value[:, :128]
            stage[2 * pair_at + 1] = value[:, 128:]

        def turn(at, carry):
            channel = pl.multiple_of(at * 8, 8)
            target[pl.ds(channel, 8)] = jnp.swapaxes(stage[:16, pl.ds(channel, 8), :], 0, 1).astype(
                jnp.bfloat16
            )
            return carry

        lax.fori_loop(0, 16, turn, 0)

    for half in range(2):
        with jax.named_scope("wait_pair"):
            pair_loads[half].wait()

        def left_rows(at, carry):
            start = pl.multiple_of(at * 16, 16)
            factor(0, half * 32 + start, left_send.at[half, :, pl.ds(start, 16)])
            return carry

        with jax.named_scope("left_rows"):
            lax.fori_loop(0, 2, left_rows, 0)
        if half == 0:
            with jax.named_scope("wait_barrier"):
                pl.semaphore_wait(barrier, 127)

        with jax.named_scope("send_left"):
            for o in ORDER:
                to = partner(o)
                send(
                    left_send.at[half, to[0] * 8 + to[1]],
                    lines.at[pl.ds(pl.multiple_of(row + half * 32, 32), 32), pl.ds(column, 128)],
                    half,
                    to,
                )

    def right_rows(at, carry):
        start = pl.multiple_of(at * 16, 16)
        factor(2, start, right_send.at[:, pl.ds(start, 16)])
        return carry

    with jax.named_scope("right_rows"):
        lax.fori_loop(0, 4, right_rows, 0)

    with jax.named_scope("send_right"):
        for parity in (0, 1):
            for o in SIDES[parity]:
                to = partner(o)
                send(
                    right_send.at[to[0] * 8 + to[1]],
                    strips.at[parity, pl.ds(row, 64), pl.ds(across, 128)],
                    2 + parity,
                    to,
                )

    lines[pl.ds(row, 32), pl.ds(column, 128)] = left_send[0, mine]
    lines[pl.ds(pl.multiple_of(row + 32, 32), 32), pl.ds(column, 128)] = left_send[1, mine]
    strips[0, pl.ds(row, 64), pl.ds(across, 128)] = right_send[mine]

    def gate_rows(at, carry):
        start = at * 4
        level = jnp.dot(
            pair[pl.ds(start, 4)].reshape(512, 128),
            weights[5],
            preferred_element_type=jnp.float32,
        )
        gate[pl.ds(start, 4)] = jax.nn.sigmoid(level).reshape(4, 128, 128)
        return carry

    with jax.named_scope("gate"):
        lax.fori_loop(0, 16, gate_rows, 0)

    def settle(ref, sem):
        pltpu.make_async_copy(ref, ref, sem).wait()

    with jax.named_scope("wait_left"):
        settle(left_send.at[0, pl.ds(0, 127)], recv_sem.at[0])
        settle(left_send.at[1, pl.ds(0, 127)], recv_sem.at[1])
    for parity in (0, 1):
        with jax.named_scope("wait_right"):
            settle(strips.at[parity, pl.ds(0, 1008 + 16 * parity)], recv_sem.at[2 + parity])

        def block(at, carry):
            start = pl.multiple_of(at * 128, 128)
            product = lax.dot_general(
                lines[:, pl.ds(start, 128)],
                strips[parity],
                (((0,), (0,)), ((), ())),
                preferred_element_type=jnp.float32,
            )
            product = (product * scale).astype(jnp.bfloat16)
            for place in range(4):
                sums[parity, place, pl.ds(start, 128)] = product[:, place * 128 : place * 128 + 128]
            return carry

        with jax.named_scope("matmul"):
            lax.fori_loop(0, 8, block, 0)

        with jax.named_scope("send_sums"):
            for first, size, index in ((0, 64, 4),) if parity == 0 else ((0, 48, 5), (48, 16, 6)):
                for o in SIDES[parity]:
                    to = partner(o)
                    start = pl.multiple_of(to[0] * 64 + first, 16)
                    send(
                        sums.at[parity, places_of[o[2]][o[0]], pl.ds(start, size)],
                        mixed.at[mine, pl.ds(first, size)],
                        index,
                        to,
                    )
    mixed[mine] = sums[0, slot, pl.ds(row, 64)]

    def finish(at, carry):
        start = at * 16 if isinstance(at, int) else pl.multiple_of(at * 16, 16)

        def turn(group, carry):
            channel = pl.multiple_of(group * 8, 8)
            stage[:, pl.ds(channel, 8), :] = jnp.swapaxes(
                mixed[pl.ds(channel, 8), pl.ds(start, 16), :].astype(jnp.float32), 0, 1
            )
            return carry

        with jax.named_scope("turn"):
            lax.fori_loop(0, 16, turn, 0)

        def line(inner, carry):
            values = stage[inner]
            centred = values - jnp.mean(values, axis=0, keepdims=True)
            spread = lax.rsqrt(jnp.mean(centred * centred, axis=0, keepdims=True) + 1e-05)
            scaled = (centred * spread * gains[...]).astype(jnp.bfloat16)
            product = lax.dot_general(
                scaled,
                weights[4],
                (((0,), (0,)), ((), ())),
                preferred_element_type=jnp.float32,
            )
            out_ref[start + inner] = (product * gate[start + inner]).astype(jnp.bfloat16)
            return carry

        with jax.named_scope("line"):
            lax.fori_loop(0, 16, line, 0, unroll=4)
        return carry

    with jax.named_scope("wait_sums"):
        settle(mixed.at[pl.ds(0, 63)], recv_sem.at[4])
        settle(mixed.at[pl.ds(0, 48)], recv_sem.at[5])
    with jax.named_scope("finish_a"):
        lax.fori_loop(0, 3, finish, 0)
    with jax.named_scope("wait_last"):
        settle(mixed.at[pl.ds(0, 16)], recv_sem.at[6])
    with jax.named_scope("finish_b"):
        finish(3, 0)

    with jax.named_scope("drain"):
        settle(left_send.at[0, pl.ds(0, 127)], send_sem.at[0])
        settle(left_send.at[1, pl.ds(0, 127)], send_sem.at[1])
        settle(strips.at[0, pl.ds(0, 1008)], send_sem.at[2])
        settle(strips.at[1], send_sem.at[3])
        settle(mixed.at[pl.ds(0, 63)], send_sem.at[4])
        settle(mixed.at[pl.ds(0, 48)], send_sem.at[5])
        settle(mixed.at[pl.ds(0, 16)], send_sem.at[6])


def on_device(
    pair_array, left_weight, right_weight, left_gate, right_gate, mid_gain, out_weight, out_gate
):
    half, single = jnp.bfloat16, jnp.float32
    call = pl.pallas_call(
        functools.partial(triangle_kernel, 1024 ** (-0.5)),
        out_shape=jax.ShapeDtypeStruct(pair_array.shape, half),
        in_specs=[pl.BlockSpec(memory_space=pltpu.HBM)] * 8,
        out_specs=pl.BlockSpec(memory_space=pltpu.VMEM),
        scratch_shapes=[
            pltpu.VMEM((64, 128, 128), half),
            pltpu.VMEM((6, 128, 128), half),
            pltpu.VMEM((1, 128), single),
            pltpu.VMEM((4, 128, 128), half),
            pltpu.VMEM((128, 128), single),
            pltpu.VMEM((16, 128, 128), single),
            pltpu.VMEM((2, 128, 32, 128), half),
            pltpu.VMEM((128, 64, 128), half),
            pltpu.VMEM((1024, 1024), half),
            pltpu.VMEM((2, 1024, 512), half),
            pltpu.VMEM((2, 4, 1024, 128), half),
            pltpu.VMEM((128, 64, 128), half),
            pltpu.VMEM((64, 128, 128), single),
            pltpu.SemaphoreType.DMA((9,)),
            pltpu.SemaphoreType.DMA((7,)),
            pltpu.SemaphoreType.DMA((7,)),
        ],
        compiler_params=pltpu.CompilerParams(
            collective_id=0, has_side_effects=True, vmem_limit_bytes=50 * 1024 * 1024
        ),
        name="triangle",
    )
    operands = (
        pair_array,
        left_weight,
        right_weight,
        left_gate,
        right_gate,
        mid_gain.reshape(1, 128),
        out_weight,
        out_gate,
    )
    return call(*(pltpu.with_memory_space_constraint(a, pltpu.HBM) for a in operands))


def solution(mesh):
    return jax.shard_map(
        on_device,
        mesh=mesh,
        in_specs=(P("pr", "pc", None), P(), P(), P(), P(), P(), P(), P()),
        out_specs=P("pr", "pc", None),
        check_vma=False,
    )
```

```python
import functools

import jax
import jax.numpy as jnp
from jax import lax
from jax.experimental import pallas as pl
from jax.experimental.pallas import tpu as pltpu
from jax.sharding import PartitionSpec as P

MESH = pl.DeviceIdType.MESH


def offsets():
    def negated(o):
        return tuple(-v % 4 for v in o)

    seen, sets = set(), []
    for code in range(64):
        o = (code // 16, code // 4 % 4, code % 4)
        if o in seen:
            continue
        one = []
        for _ in range(3):
            for p in (o, negated(o)):
                if p not in one:
                    one.append(p)
            o = (o[2], o[0], o[1])
        seen.update(one)
        sets.append(one)
    sets.sort(key=lambda one: -sum(min(v, 4 - v) for v in one[0]))
    flat = [o for one in sets for o in one]
    order = [(*o, (at + turn) % 2) for turn in (0, 1) for at, o in enumerate(flat)]
    return [o for o in order if o != (0, 0, 0, 0)]


ORDER = offsets()
PIECES = (((0, 4, 4),), ((0, 2, 5), (2, 1, 6), (3, 1, 7)))
SIDES = [[o for o in ORDER if o[0] % 2 == parity] for parity in (0, 1)]


def triangle_kernel(
    scale,
    pair_hbm,
    left_weight_hbm,
    right_weight_hbm,
    left_gate_hbm,
    right_gate_hbm,
    gain_hbm,
    out_weight_hbm,
    out_gate_hbm,
    out_ref,
    pair,
    weights,
    gain_row,
    turned,
    gains,
    stage,
    left_send,
    right_send,
    lines,
    lines_t,
    strips,
    sums,
    mixed,
    gate,
    load_sem,
    send_sem,
    recv_sem,
):
    pr, pc = lax.axis_index("pr"), lax.axis_index("pc")
    x, y, c = lax.rem(pc, 4), lax.rem(lax.div(pr, 2), 4), lax.rem(pr, 2)
    z = lax.div(pc, 4) * 2 + lax.div(pr, 8)
    mine = pr * 8 + pc
    slot = lax.div(pc, 4) * 2 + lax.div(x, 2)
    xs = [lax.rem(x + d + c * (-2 * d % 4), 4) for d in range(4)]
    ys = [lax.rem(y + d + c * (-2 * d % 4), 4) * 2 for d in range(4)]
    zs = [lax.rem(z + d + c * (-2 * d % 4), 4) for d in range(4)]
    rows_of = [[lax.rem(v, 2) * 8 + w for w in ys] for v in zs]
    columns_of = [[lax.div(v, 2) * 4 + w for w in xs] for v in zs]
    places_of = [[lax.div(v, 2) * 2 + lax.div(w, 2) for w in xs] for v in zs]
    cores = [c, 1 - c]

    def partner(o):
        dx, dy, dz, dc = o
        return rows_of[dz][dy] + cores[dc], columns_of[dz][dx]

    row, column = pl.multiple_of(pr * 64, 64), pl.multiple_of(pc * 128, 128)
    across = pl.multiple_of(slot * 128, 128)

    matrices = (
        left_weight_hbm,
        left_gate_hbm,
        right_weight_hbm,
        right_gate_hbm,
        out_weight_hbm,
        out_gate_hbm,
    )
    loads = [
        pltpu.make_async_copy(ref, weights.at[index], load_sem.at[index])
        for index, ref in enumerate(matrices)
    ]
    loads.append(pltpu.make_async_copy(gain_hbm, gain_row, load_sem.at[6]))
    pair_loads = [
        pltpu.make_async_copy(
            pair_hbm.at[pl.ds(first, 32)], pair.at[pl.ds(first, 32)], load_sem.at[7 + first // 32]
        )
        for first in (0, 32)
    ]
    for load in loads + pair_loads:
        load.start()
    barrier = pltpu.get_barrier_semaphore()

    with jax.named_scope("greet"):
        for o in ORDER:
            pl.semaphore_signal(barrier, inc=1, device_id=partner(o), device_id_type=MESH)

    def send(source, target, index, to):
        pltpu.make_async_remote_copy(
            source, target, send_sem.at[index], recv_sem.at[index], device_id=to, device_id_type=MESH
        ).start()

    with jax.named_scope("weights"):
        for load in loads:
            load.wait()
        for index in range(4):
            turned[index] = weights[index].astype(jnp.float32).T.astype(jnp.bfloat16)
        gains[...] = jnp.broadcast_to(gain_row[...], (128, 128)).T

    def factor(index, first, target):
        for pair_at in range(8):
            both = pair[pl.ds(first + 2 * pair_at, 2)].reshape(256, 128)
            value = lax.dot_general(
                turned[index], both, (((1,), (1,)), ((), ())), preferred_element_type=jnp.float32
            )
            level = lax.dot_general(
                turned[index + 1], both, (((1,), (1,)), ((), ())), preferred_element_type=jnp.float32
            )
            value = value * jax.nn.sigmoid(level)
            stage[2 * pair_at] = value[:, :128]
            stage[2 * pair_at + 1] = value[:, 128:]

        def turn(at, carry):
            channel = pl.multiple_of(at * 8, 8)
            target[pl.ds(channel, 8)] = jnp.swapaxes(stage[:16, pl.ds(channel, 8), :], 0, 1).astype(
                jnp.bfloat16
            )
            return carry

        lax.fori_loop(0, 16, turn, 0)

    for half in range(2):
        with jax.named_scope("wait_pair"):
            pair_loads[half].wait()

        def left_rows(at, carry):
            start = pl.multiple_of(at * 16, 16)
            factor(0, half * 32 + start, left_send.at[half, :, pl.ds(start, 16)])
            return carry

        with jax.named_scope("left_rows"):
            lax.fori_loop(0, 2, left_rows, 0)
        if half == 0:
            with jax.named_scope("wait_barrier"):
                pl.semaphore_wait(barrier, 127)

        with jax.named_scope("send_left"):
            for o in ORDER:
                to = partner(o)
                send(
                    left_send.at[half, to[0] * 8 + to[1]],
                    lines.at[pl.ds(pl.multiple_of(row + half * 32, 32), 32), pl.ds(column, 128)],
                    half,
                    to,
                )

    def right_rows(at, carry):
        start = pl.multiple_of(at * 16, 16)
        factor(2, start, right_send.at[:, pl.ds(start, 16)])
        return carry

    with jax.named_scope("right_rows"):
        lax.fori_loop(0, 4, right_rows, 0)

    with jax.named_scope("send_right"):
        for parity in (0, 1):
            for o in SIDES[parity]:
                to = partner(o)
                send(
                    right_send.at[to[0] * 8 + to[1]],
                    strips.at[parity, pl.ds(row, 64), pl.ds(across, 128)],
                    2 + parity,
                    to,
                )

    lines[pl.ds(row, 32), pl.ds(column, 128)] = left_send[0, mine]
    lines[pl.ds(pl.multiple_of(row + 32, 32), 32), pl.ds(column, 128)] = left_send[1, mine]
    strips[0, pl.ds(row, 64), pl.ds(across, 128)] = right_send[mine]

    def gate_rows(at, carry):
        start = at * 4
        level = jnp.dot(
            pair[pl.ds(start, 4)].reshape(512, 128),
            weights[5],
            preferred_element_type=jnp.float32,
        )
        gate[pl.ds(start, 4)] = jax.nn.sigmoid(level).reshape(4, 128, 128)
        return carry

    with jax.named_scope("gate"):
        lax.fori_loop(0, 16, gate_rows, 0)

    def settle(ref, sem):
        pltpu.make_async_copy(ref, ref, sem).wait()

    with jax.named_scope("wait_left"):
        settle(left_send.at[0, pl.ds(0, 127)], recv_sem.at[0])
        settle(left_send.at[1, pl.ds(0, 127)], recv_sem.at[1])
    def turn_lines(at, carry):
        block = lines[:, pl.ds(pl.multiple_of(at * 128, 128), 128)].T.reshape(2, 4, 16, 1024)
        for quarter in range(4):
            lines_t[quarter, pl.ds(at * 2, 2)] = block[:, quarter]
        return carry

    with jax.named_scope("turn_lines"):
        lax.fori_loop(0, 8, turn_lines, 0)

    for parity in (0, 1):
        with jax.named_scope("wait_right"):
            settle(strips.at[parity, pl.ds(0, 1008 + 16 * parity)], recv_sem.at[2 + parity])

        def block(at, carry):
            quarter, group = lax.div(at, 2), lax.rem(at, 2) * 8
            product = jnp.dot(
                lines_t[quarter, pl.ds(group, 8)].reshape(128, 1024),
                strips[parity],
                preferred_element_type=jnp.float32,
            )
            product = (product * scale).astype(jnp.bfloat16)
            for place in range(4):
                sums[parity, quarter, place, pl.ds(group, 8)] = product[
                    :, place * 128 : place * 128 + 128
                ].reshape(8, 16, 128)
            return carry

        for first, size, index in PIECES[parity]:
            with jax.named_scope("matmul"):
                lax.fori_loop(2 * first, 2 * (first + size), block, 0)
            with jax.named_scope("send_sums"):
                for o in SIDES[parity]:
                    to = partner(o)
                    send(
                        sums.at[parity, pl.ds(first, size), places_of[o[2]][o[0]], to[0]],
                        mixed.at[mine, pl.ds(first, size)],
                        index,
                        to,
                    )
    for quarter in range(4):
        mixed[mine, quarter] = sums[0, quarter, slot, pr]

    def finish(at, carry):
        start = at * 16 if isinstance(at, int) else pl.multiple_of(at * 16, 16)

        def turn(group, carry):
            channel = pl.multiple_of(group * 8, 8)
            stage[:, pl.ds(channel, 8), :] = jnp.swapaxes(
                mixed[pl.ds(channel, 8), at].astype(jnp.float32), 0, 1
            )
            return carry

        with jax.named_scope("turn"):
            lax.fori_loop(0, 16, turn, 0, unroll=8)

        def line(inner, carry):
            values = stage[inner]
            centred = values - jnp.mean(values, axis=0, keepdims=True)
            spread = lax.rsqrt(jnp.mean(centred * centred, axis=0, keepdims=True) + 1e-05)
            scaled = (centred * spread * gains[...]).astype(jnp.bfloat16)
            product = lax.dot_general(
                scaled,
                weights[4],
                (((0,), (0,)), ((), ())),
                preferred_element_type=jnp.float32,
            )
            out_ref[start + inner] = (product * gate[start + inner]).astype(jnp.bfloat16)
            return carry

        with jax.named_scope("line"):
            lax.fori_loop(0, 16, line, 0, unroll=16)
        return carry

    with jax.named_scope("wait_sums"):
        settle(mixed.at[pl.ds(0, 63)], recv_sem.at[4])
    for first, size, index in PIECES[1]:
        with jax.named_scope("wait_piece"):
            settle(mixed.at[pl.ds(0, 16 * size)], recv_sem.at[index])
        with jax.named_scope("finish"):
            lax.fori_loop(first, first + size, finish, 0)

    with jax.named_scope("drain"):
        settle(left_send.at[0, pl.ds(0, 127)], send_sem.at[0])
        settle(left_send.at[1, pl.ds(0, 127)], send_sem.at[1])
        settle(strips.at[0, pl.ds(0, 1008)], send_sem.at[2])
        settle(strips.at[1], send_sem.at[3])
        settle(mixed.at[pl.ds(0, 63)], send_sem.at[4])
        for _, size, index in PIECES[1]:
            settle(mixed.at[pl.ds(0, 16 * size)], send_sem.at[index])


def on_device(
    pair_array, left_weight, right_weight, left_gate, right_gate, mid_gain, out_weight, out_gate
):
    half, single = jnp.bfloat16, jnp.float32
    call = pl.pallas_call(
        functools.partial(triangle_kernel, 1024 ** (-0.5)),
        out_shape=jax.ShapeDtypeStruct(pair_array.shape, half),
        in_specs=[pl.BlockSpec(memory_space=pltpu.HBM)] * 8,
        out_specs=pl.BlockSpec(memory_space=pltpu.VMEM),
        scratch_shapes=[
            pltpu.VMEM((64, 128, 128), half),
            pltpu.VMEM((6, 128, 128), half),
            pltpu.VMEM((1, 128), single),
            pltpu.VMEM((4, 128, 128), half),
            pltpu.VMEM((128, 128), single),
            pltpu.VMEM((16, 128, 128), single),
            pltpu.VMEM((2, 128, 32, 128), half),
            pltpu.VMEM((128, 64, 128), half),
            pltpu.VMEM((1024, 1024), half),
            pltpu.VMEM((4, 16, 16, 1024), half),
            pltpu.VMEM((2, 1024, 512), half),
            pltpu.VMEM((2, 4, 4, 16, 16, 128), half),
            pltpu.VMEM((128, 4, 16, 128), half),
            pltpu.VMEM((64, 128, 128), single),
            pltpu.SemaphoreType.DMA((9,)),
            pltpu.SemaphoreType.DMA((8,)),
            pltpu.SemaphoreType.DMA((8,)),
        ],
        compiler_params=pltpu.CompilerParams(
            collective_id=0, has_side_effects=True, vmem_limit_bytes=50 * 1024 * 1024
        ),
        name="triangle",
    )
    operands = (
        pair_array,
        left_weight,
        right_weight,
        left_gate,
        right_gate,
        mid_gain.reshape(1, 128),
        out_weight,
        out_gate,
    )
    return call(*(pltpu.with_memory_space_constraint(a, pltpu.HBM) for a in operands))


def solution(mesh):
    return jax.shard_map(
        on_device,
        mesh=mesh,
        in_specs=(P("pr", "pc", None), P(), P(), P(), P(), P(), P(), P()),
        out_specs=P("pr", "pc", None),
        check_vma=False,
    )
```

```python
import functools

import jax
import jax.numpy as jnp
from jax import lax
from jax.experimental import pallas as pl
from jax.experimental.pallas import tpu as pltpu
from jax.sharding import PartitionSpec as P

MESH = pl.DeviceIdType.MESH


def offsets():
    def negated(o):
        return tuple(-v % 4 for v in o)

    seen, sets = set(), []
    for code in range(64):
        o = (code // 16, code // 4 % 4, code % 4)
        if o in seen:
            continue
        one = []
        for _ in range(3):
            for p in (o, negated(o)):
                if p not in one:
                    one.append(p)
            o = (o[2], o[0], o[1])
        seen.update(one)
        sets.append(one)
    sets.sort(key=lambda one: -sum(min(v, 4 - v) for v in one[0]))
    flat = [o for one in sets for o in one]
    order = [(*o, (at + turn) % 2) for turn in (0, 1) for at, o in enumerate(flat)]
    return [o for o in order if o != (0, 0, 0, 0)]


ORDER = offsets()
PIECES = (((0, 4, 4),), ((0, 2, 5), (2, 1, 6), (3, 1, 7)))
SIDES = [[o for o in ORDER if o[0] % 2 == parity] for parity in (0, 1)]


def finish_rows(at, mixed_rows, gate_rows, out_weight, gains, stage, out_rows):
    def turn(group, carry):
        channel = pl.multiple_of(group * 8, 8)
        stage[:, pl.ds(channel, 8), :] = jnp.swapaxes(
            mixed_rows[pl.ds(channel, 8)].astype(jnp.float32), 0, 1
        )
        return carry

    lax.fori_loop(0, 16, turn, 0, unroll=8)

    def line(inner, carry):
        values = stage[inner]
        centred = values - jnp.mean(values, axis=0, keepdims=True)
        spread = lax.rsqrt(jnp.mean(centred * centred, axis=0, keepdims=True) + 1e-05)
        scaled = (centred * spread * gains[...]).astype(jnp.bfloat16)
        product = lax.dot_general(
            scaled, out_weight[...], (((0,), (0,)), ((), ())), preferred_element_type=jnp.float32
        )
        out_rows[at + inner] = (product * gate_rows[at + inner]).astype(jnp.bfloat16)
        return carry

    lax.fori_loop(0, 16, line, 0, unroll=16)


def last_kernel(rows_ref, mixed, gate, out_weight, gains, out_hbm, stage, last, sems):
    first = pltpu.make_async_copy(rows_ref, out_hbm.at[pl.ds(0, 48)], sems.at[0])
    first.start()
    finish_rows(0, mixed.at[:, 3], gate.at[pl.ds(48, 16)], out_weight, gains, stage, last)
    second = pltpu.make_async_copy(last, out_hbm.at[pl.ds(48, 16)], sems.at[1])
    second.start()
    first.wait()
    second.wait()


def triangle_kernel(
    scale,
    pair_hbm,
    left_weight_hbm,
    right_weight_hbm,
    left_gate_hbm,
    right_gate_hbm,
    gain_hbm,
    out_weight_hbm,
    out_gate_hbm,
    out_ref,
    mixed,
    gate,
    weight_ref,
    gains,
    pair,
    weights,
    gain_row,
    turned,
    stage,
    left_send,
    right_send,
    lines,
    lines_t,
    strips,
    sums,
    load_sem,
    send_sem,
    recv_sem,
):
    pr, pc = lax.axis_index("pr"), lax.axis_index("pc")
    x, y, c = lax.rem(pc, 4), lax.rem(lax.div(pr, 2), 4), lax.rem(pr, 2)
    z = lax.div(pc, 4) * 2 + lax.div(pr, 8)
    mine = pr * 8 + pc
    slot = lax.div(pc, 4) * 2 + lax.div(x, 2)
    xs = [lax.rem(x + d + c * (-2 * d % 4), 4) for d in range(4)]
    ys = [lax.rem(y + d + c * (-2 * d % 4), 4) * 2 for d in range(4)]
    zs = [lax.rem(z + d + c * (-2 * d % 4), 4) for d in range(4)]
    rows_of = [[lax.rem(v, 2) * 8 + w for w in ys] for v in zs]
    columns_of = [[lax.div(v, 2) * 4 + w for w in xs] for v in zs]
    places_of = [[lax.div(v, 2) * 2 + lax.div(w, 2) for w in xs] for v in zs]
    cores = [c, 1 - c]

    def partner(o):
        dx, dy, dz, dc = o
        return rows_of[dz][dy] + cores[dc], columns_of[dz][dx]

    row, column = pl.multiple_of(pr * 64, 64), pl.multiple_of(pc * 128, 128)
    across = pl.multiple_of(slot * 128, 128)

    matrices = (
        left_weight_hbm,
        left_gate_hbm,
        right_weight_hbm,
        right_gate_hbm,
        out_weight_hbm,
        out_gate_hbm,
    )
    loads = [
        pltpu.make_async_copy(ref, weights.at[index], load_sem.at[index])
        for index, ref in enumerate(matrices)
    ]
    loads.append(pltpu.make_async_copy(gain_hbm, gain_row, load_sem.at[6]))
    pair_loads = [
        pltpu.make_async_copy(
            pair_hbm.at[pl.ds(first, 32)], pair.at[pl.ds(first, 32)], load_sem.at[7 + first // 32]
        )
        for first in (0, 32)
    ]
    for load in loads + pair_loads:
        load.start()
    barrier = pltpu.get_barrier_semaphore()

    with jax.named_scope("greet"):
        for o in ORDER:
            pl.semaphore_signal(barrier, inc=1, device_id=partner(o), device_id_type=MESH)

    def send(source, target, index, to):
        pltpu.make_async_remote_copy(
            source, target, send_sem.at[index], recv_sem.at[index], device_id=to, device_id_type=MESH
        ).start()

    with jax.named_scope("weights"):
        for load in loads:
            load.wait()
        for index in range(4):
            turned[index] = weights[index].astype(jnp.float32).T.astype(jnp.bfloat16)
        gains[...] = jnp.broadcast_to(gain_row[...], (128, 128)).T

    def factor(index, first, target):
        for pair_at in range(8):
            both = pair[pl.ds(first + 2 * pair_at, 2)].reshape(256, 128)
            value = lax.dot_general(
                turned[index], both, (((1,), (1,)), ((), ())), preferred_element_type=jnp.float32
            )
            level = lax.dot_general(
                turned[index + 1], both, (((1,), (1,)), ((), ())), preferred_element_type=jnp.float32
            )
            value = value * jax.nn.sigmoid(level)
            stage[2 * pair_at] = value[:, :128]
            stage[2 * pair_at + 1] = value[:, 128:]

        def turn(at, carry):
            channel = pl.multiple_of(at * 8, 8)
            target[pl.ds(channel, 8)] = jnp.swapaxes(stage[:16, pl.ds(channel, 8), :], 0, 1).astype(
                jnp.bfloat16
            )
            return carry

        lax.fori_loop(0, 16, turn, 0)

    for half in range(2):
        with jax.named_scope("wait_pair"):
            pair_loads[half].wait()

        def left_rows(at, carry):
            start = pl.multiple_of(at * 16, 16)
            factor(0, half * 32 + start, left_send.at[half, :, pl.ds(start, 16)])
            return carry

        with jax.named_scope("left_rows"):
            lax.fori_loop(0, 2, left_rows, 0)
        if half == 0:
            with jax.named_scope("wait_barrier"):
                pl.semaphore_wait(barrier, 127)

        with jax.named_scope("send_left"):
            for o in ORDER:
                to = partner(o)
                send(
                    left_send.at[half, to[0] * 8 + to[1]],
                    lines.at[pl.ds(pl.multiple_of(row + half * 32, 32), 32), pl.ds(column, 128)],
                    half,
                    to,
                )

    def right_rows(at, carry):
        start = pl.multiple_of(at * 16, 16)
        factor(2, start, right_send.at[:, pl.ds(start, 16)])
        return carry

    with jax.named_scope("right_rows"):
        lax.fori_loop(0, 4, right_rows, 0)

    with jax.named_scope("send_right"):
        for parity in (0, 1):
            for o in SIDES[parity]:
                to = partner(o)
                send(
                    right_send.at[to[0] * 8 + to[1]],
                    strips.at[parity, pl.ds(row, 64), pl.ds(across, 128)],
                    2 + parity,
                    to,
                )

    lines[pl.ds(row, 32), pl.ds(column, 128)] = left_send[0, mine]
    lines[pl.ds(pl.multiple_of(row + 32, 32), 32), pl.ds(column, 128)] = left_send[1, mine]
    strips[0, pl.ds(row, 64), pl.ds(across, 128)] = right_send[mine]

    def gate_rows(at, carry):
        start = at * 4
        level = jnp.dot(
            pair[pl.ds(start, 4)].reshape(512, 128),
            weights[5],
            preferred_element_type=jnp.float32,
        )
        gate[pl.ds(start, 4)] = jax.nn.sigmoid(level).reshape(4, 128, 128)
        return carry

    with jax.named_scope("gate"):
        lax.fori_loop(0, 16, gate_rows, 0)

    def settle(ref, sem):
        pltpu.make_async_copy(ref, ref, sem).wait()

    with jax.named_scope("wait_left"):
        settle(left_send.at[0, pl.ds(0, 127)], recv_sem.at[0])
        settle(left_send.at[1, pl.ds(0, 127)], recv_sem.at[1])
    def turn_lines(at, carry):
        block = lines[:, pl.ds(pl.multiple_of(at * 128, 128), 128)].T.reshape(2, 4, 16, 1024)
        for quarter in range(4):
            lines_t[quarter, pl.ds(at * 2, 2)] = block[:, quarter]
        return carry

    with jax.named_scope("turn_lines"):
        lax.fori_loop(0, 8, turn_lines, 0)

    for parity in (0, 1):
        with jax.named_scope("wait_right"):
            settle(strips.at[parity, pl.ds(0, 1008 + 16 * parity)], recv_sem.at[2 + parity])

        def block(at, carry):
            quarter, group = lax.div(at, 2), lax.rem(at, 2) * 8
            product = jnp.dot(
                lines_t[quarter, pl.ds(group, 8)].reshape(128, 1024),
                strips[parity],
                preferred_element_type=jnp.float32,
            )
            product = (product * scale).astype(jnp.bfloat16)
            for place in range(4):
                sums[parity, quarter, place, pl.ds(group, 8)] = product[
                    :, place * 128 : place * 128 + 128
                ].reshape(8, 16, 128)
            return carry

        for first, size, index in PIECES[parity]:
            with jax.named_scope("matmul"):
                lax.fori_loop(2 * first, 2 * (first + size), block, 0)
            with jax.named_scope("send_sums"):
                for o in SIDES[parity]:
                    to = partner(o)
                    send(
                        sums.at[parity, pl.ds(first, size), places_of[o[2]][o[0]], to[0]],
                        mixed.at[mine, pl.ds(first, size)],
                        index,
                        to,
                    )
    for quarter in range(4):
        mixed[mine, quarter] = sums[0, quarter, slot, pr]

    def finish(at, carry):
        start = pl.multiple_of(at * 16, 16)
        finish_rows(start, mixed.at[:, at], gate, weights.at[4], gains, stage, out_ref)
        return carry

    with jax.named_scope("wait_sums"):
        settle(mixed.at[pl.ds(0, 63)], recv_sem.at[4])
    for first, size, index in PIECES[1]:
        with jax.named_scope("wait_piece"):
            settle(mixed.at[pl.ds(0, 16 * size)], recv_sem.at[index])
        if first < 3:
            with jax.named_scope("finish"):
                lax.fori_loop(first, first + size, finish, 0)
    weight_ref[...] = weights[4]

    with jax.named_scope("drain"):
        settle(left_send.at[0, pl.ds(0, 127)], send_sem.at[0])
        settle(left_send.at[1, pl.ds(0, 127)], send_sem.at[1])
        settle(strips.at[0, pl.ds(0, 1008)], send_sem.at[2])
        settle(strips.at[1], send_sem.at[3])
        settle(mixed.at[pl.ds(0, 63)], send_sem.at[4])
        for _, size, index in PIECES[1]:
            settle(mixed.at[pl.ds(0, 16 * size)], send_sem.at[index])


def on_device(
    pair_array, left_weight, right_weight, left_gate, right_gate, mid_gain, out_weight, out_gate
):
    half, single = jnp.bfloat16, jnp.float32
    call = pl.pallas_call(
        functools.partial(triangle_kernel, 1024 ** (-0.5)),
        out_shape=(
            jax.ShapeDtypeStruct((48, 128, 128), half),
            jax.ShapeDtypeStruct((128, 4, 16, 128), half),
            jax.ShapeDtypeStruct((64, 128, 128), single),
            jax.ShapeDtypeStruct((128, 128), half),
            jax.ShapeDtypeStruct((128, 128), single),
        ),
        in_specs=[pl.BlockSpec(memory_space=pltpu.HBM)] * 8,
        out_specs=[pl.BlockSpec(memory_space=pltpu.VMEM)] * 5,
        scratch_shapes=[
            pltpu.VMEM((64, 128, 128), half),
            pltpu.VMEM((6, 128, 128), half),
            pltpu.VMEM((1, 128), single),
            pltpu.VMEM((4, 128, 128), half),
            pltpu.VMEM((16, 128, 128), single),
            pltpu.VMEM((2, 128, 32, 128), half),
            pltpu.VMEM((128, 64, 128), half),
            pltpu.VMEM((1024, 1024), half),
            pltpu.VMEM((4, 16, 16, 1024), half),
            pltpu.VMEM((2, 1024, 512), half),
            pltpu.VMEM((2, 4, 4, 16, 16, 128), half),
            pltpu.SemaphoreType.DMA((9,)),
            pltpu.SemaphoreType.DMA((8,)),
            pltpu.SemaphoreType.DMA((8,)),
        ],
        compiler_params=pltpu.CompilerParams(
            collective_id=0, has_side_effects=True, vmem_limit_bytes=40 * 1024 * 1024
        ),
        name="triangle",
    )
    operands = (
        pair_array,
        left_weight,
        right_weight,
        left_gate,
        right_gate,
        mid_gain.reshape(1, 128),
        out_weight,
        out_gate,
    )
    parts = call(*(pltpu.with_memory_space_constraint(a, pltpu.HBM) for a in operands))
    return pl.pallas_call(
        last_kernel,
        out_shape=jax.ShapeDtypeStruct(pair_array.shape, half),
        in_specs=[pl.BlockSpec(memory_space=pltpu.VMEM)] * 5,
        out_specs=pl.BlockSpec(memory_space=pltpu.HBM),
        scratch_shapes=[
            pltpu.VMEM((16, 128, 128), single),
            pltpu.VMEM((16, 128, 128), half),
            pltpu.SemaphoreType.DMA((2,)),
        ],
        compiler_params=pltpu.CompilerParams(vmem_limit_bytes=16 * 1024 * 1024),
        name="last_rows",
    )(*parts)


def solution(mesh):
    return jax.shard_map(
        on_device,
        mesh=mesh,
        in_specs=(P("pr", "pc", None), P(), P(), P(), P(), P(), P(), P()),
        out_specs=P("pr", "pc", None),
        check_vma=False,
    )
```
